8 devices in a mesh: dp: 2 (over y, z), tp: 4 (over x, core).
Axes of the slice: x: 2, y: 2, z: 1, core: 2. Of those that a mesh axis runs over, the one named last changes fastest.
Arguments:
- x: bfloat16 [4096, 4096], P('dp'), parts along dimension 0
- w_gate: bfloat16 [4096, 12800], P(None, 'tp')
- w_up: bfloat16 [4096, 12800], P(None, 'tp')
- w_down: bfloat16 [12800, 4096], P('tp')
Outputs:
- output: bfloat16 [4096, 4096], P('dp'), parts along dimension 0
There are 2 independent parts. The reference program is written for one: setup_inputs(seed, part) draws one part's arguments, and reference() takes and returns one part's arrays. A program takes and returns all parts, laid end to end along the dimension named above; an argument that names none is the same for every part.
All inputs are finite; a program needn't handle non-finite values.
Results may differ from the reference program's by a relative error of at most 0.016.
Values are sent between devices in bfloat16 or wider.
A program may use at most 2 GiB of HBM per device.

```python
import jax
import jax.numpy as jnp

ROWS = 2048
D = 4096
FF = 12800


def setup_inputs(seed: int = 0, part: int = 0) -> dict:
    kx, kg, ku, kd = jax.random.split(jax.random.key(seed), 4)
    drawn = {
        "x": jax.random.normal(jax.random.fold_in(kx, part), (ROWS, D), jnp.float32),
        "w_gate": jax.random.normal(kg, (D, FF), jnp.float32) * D**-0.5,
        "w_up": jax.random.normal(ku, (D, FF), jnp.float32) * D**-0.5,
        "w_down": jax.random.normal(kd, (FF, D), jnp.float32) * FF**-0.5,
    }
    return {k: v.astype(jnp.bfloat16) for k, v in drawn.items()}


def reference(x, w_gate, w_up, w_down):
    gate = jnp.dot(x, w_gate, preferred_element_type=jnp.float32)
    up = jnp.dot(x, w_up, preferred_element_type=jnp.float32)
    hidden = (jax.nn.silu(gate) * up).astype(jnp.bfloat16)
    return jnp.dot(hidden, w_down, preferred_element_type=jnp.float32).astype(jnp.bfloat16)
```

```python
import jax
import jax.numpy as jnp
from jax import lax
from jax.experimental import pallas as pl
from jax.experimental.pallas import tpu as pltpu
from jax.sharding import PartitionSpec as P

R = 256
TG = 640
TD = 512
F32, BF16 = jnp.float32, jnp.bfloat16


def mlp_kernel(
    x_hbm, wg_hbm, wu_hbm, wd_hbm, y_hbm,
    x_v, w_v, wd_v, h_v, own_v, sout_v, sin_v, xout_v, xin_v, fin_v,
    x_sem, w_sem, wd_sem, s_send, s_recv, c_send, c_recv, f_send, f_recv, l_sem, s_free, c_free,
):
    rows, d = x_hbm.shape
    ff = wg_hbm.shape[1]
    nb, ng, half = rows // R, ff // TG, d // 2
    nd = half // TD
    tp = lax.axis_index("tp")
    core = lax.rem(tp, 2)
    sib = tp + 1 - 2 * core
    far = lax.rem(tp + 2, 4)
    nsin, nx = sin_v.shape[0], xout_v.shape[0]

    def x_copy(b):
        return pltpu.make_async_copy(
            x_hbm.at[pl.ds(pl.multiple_of(b * R, R), R), :], x_v.at[lax.rem(b, 2)], x_sem.at[lax.rem(b, 2)])

    def w_copies(t):
        slot = lax.rem(t, 2)
        cols = pl.ds(pl.multiple_of(lax.rem(t, ng) * TG, 128), TG)
        return (
            pltpu.make_async_copy(wg_hbm.at[:, cols], w_v.at[slot, :, pl.ds(0, TG)], w_sem.at[slot, 0]),
            pltpu.make_async_copy(wu_hbm.at[:, cols], w_v.at[slot, :, pl.ds(TG, TG)], w_sem.at[slot, 1]),
        )

    def wd_copy(j):
        cols = pl.ds(pl.multiple_of(j * TD, TD), TD)
        return pltpu.make_async_copy(wd_hbm.at[:, cols], wd_v.at[j], wd_sem.at[j])

    def s_copy(k):
        return pltpu.make_async_remote_copy(
            src_ref=sout_v.at[lax.rem(k, 2)], dst_ref=sin_v.at[lax.rem(k, nsin)],
            send_sem=s_send.at[lax.rem(k, 2)], recv_sem=s_recv.at[lax.rem(k, nsin)],
            device_id={"tp": sib}, device_id_type=pl.DeviceIdType.MESH)

    def c_copy(k):
        slot = lax.rem(k, nx)
        return pltpu.make_async_remote_copy(
            src_ref=xout_v.at[slot], dst_ref=xin_v.at[slot], send_sem=c_send.at[slot], recv_sem=c_recv.at[slot],
            device_id={"tp": far}, device_id_type=pl.DeviceIdType.MESH)

    def y_at(k):
        b, s = k // nd, lax.rem(k, nd)
        return y_hbm.at[pl.ds(pl.multiple_of(b * R, R), R), pl.ds(pl.multiple_of(core * half + s * TD, TD), TD)]

    def f_copies(k):
        slot = lax.rem(k, 2)
        return (
            pltpu.make_async_remote_copy(
                src_ref=fin_v.at[slot], dst_ref=y_at(k), send_sem=f_send.at[slot], recv_sem=f_recv,
                device_id={"tp": sib}, device_id_type=pl.DeviceIdType.MESH),
            pltpu.make_async_copy(fin_v.at[slot], y_at(k), l_sem.at[slot]),
        )

    def chip_sum(k):
        s_copy(k).wait_recv()
        slot = lax.rem(k, nx)
        xout_v[slot] = (own_v[lax.rem(k, 2)] + sin_v[lax.rem(k, nsin)].astype(F32)).astype(BF16)

        @pl.when(k + nsin < nb * nd)
        def _():
            pl.semaphore_signal(s_free, inc=1, device_id={"tp": sib}, device_id_type=pl.DeviceIdType.MESH)

        @pl.when(k >= nx)
        def _():
            pl.semaphore_wait(c_free, 1)

        c_copy(k).start()

    def finish(k):
        @pl.when(k >= 2)
        def _():
            remote, local = f_copies(k - 2)
            remote.wait_send()
            local.wait()

        copy = c_copy(k)
        copy.wait_send()
        copy.wait_recv()
        slot = lax.rem(k, nx)
        fin_v[lax.rem(k, 2)] = (xout_v[slot].astype(F32) + xin_v[slot].astype(F32)).astype(BF16)

        @pl.when(k + nx < nb * nd)
        def _():
            pl.semaphore_signal(c_free, inc=1, device_id={"tp": far}, device_id_type=pl.DeviceIdType.MESH)

        remote, local = f_copies(k)
        remote.start()
        local.start()

    x_copy(0).start()
    for t in range(2):
        for c in w_copies(t):
            c.start()

    barrier = pltpu.get_barrier_semaphore()
    for other in (sib, far):
        pl.semaphore_signal(barrier, inc=1, device_id={"tp": other}, device_id_type=pl.DeviceIdType.MESH)
    pl.semaphore_wait(barrier, 2)

    def block(b, _):
        x_copy(b).wait()

        @pl.when(b + 1 < nb)
        def _():
            x_copy(b + 1).start()

        def up_stage(g, _):
            t = b * ng + g
            slot = lax.rem(t, 2)
            for c in w_copies(t):
                c.wait()

            gu = jnp.dot(x_v[lax.rem(b, 2)], w_v[slot], preferred_element_type=F32)
            gate, up = gu[:, :TG], gu[:, TG:]
            cols = pl.ds(pl.multiple_of(g * TG, 128), TG)
            h_v[:, cols] = (gate * jax.nn.sigmoid(gate) * up).astype(BF16)

            @pl.when((b == 0) & (g == 2))
            def _():
                for s in range(nd):
                    wd_copy((1 - core) * nd + s).start()
                    wd_copy(core * nd + s).start()

            @pl.when(t + 2 < nb * ng)
            def _():
                for c in w_copies(t + 2):
                    c.start()

            @pl.when((b > 0) & (g == 0))
            def _():
                chip_sum(b * nd - 1)

            @pl.when((b > 0) & ((g == 2) | (g == 4)))
            def _():
                finish((b - 1) * nd + g // 2 - 1)

            return 0

        lax.fori_loop(0, ng, up_stage, 0)

        def down_stage(s, _):
            k = b * nd + s
            js, jo = (1 - core) * nd + s, core * nd + s

            @pl.when(b == 0)
            def _():
                wd_copy(js).wait()
                wd_copy(jo).wait()

            @pl.when(k >= 2)
            def _():
                s_copy(k - 2).wait_send()

            sout_v[lax.rem(k, 2)] = jnp.dot(h_v[...], wd_v[js], preferred_element_type=F32).astype(BF16)
            own_v[lax.rem(k, 2)] = jnp.dot(h_v[...], wd_v[jo], preferred_element_type=F32)

            @pl.when(k >= nsin)
            def _():
                pl.semaphore_wait(s_free, 1)

            s_copy(k).start()

            @pl.when(s > 0)
            def _():
                chip_sum(k - 1)

            @pl.when((b > 0) & ((s == 1) | (s == 3)))
            def _():
                finish((b - 1) * nd + 2 + s // 2)

            return 0

        lax.fori_loop(0, nd, down_stage, 0)
        return 0

    lax.fori_loop(0, nb, block, 0)

    last = nb * nd
    chip_sum(last - 1)

    def tail(k, _):
        finish(k)
        return 0

    lax.fori_loop(last - nd, last, tail, 0)
    for k in (last - 2, last - 1):
        s_copy(k).wait_send()
        remote, local = f_copies(k)
        remote.wait_send()
        local.wait()
    theirs = y_hbm.at[:, pl.ds(pl.multiple_of((1 - core) * half, half), half)]
    pltpu.make_async_remote_copy(
        src_ref=theirs, dst_ref=theirs, send_sem=f_send.at[0], recv_sem=f_recv,
        device_id={"tp": sib}, device_id_type=pl.DeviceIdType.MESH).wait_recv()


def solution(mesh):
    def step(x, w_gate, w_up, w_down):
        rows, d = x.shape
        ff = w_gate.shape[1]
        chunk = (R, TD)
        dma = pltpu.SemaphoreType.DMA
        return pl.pallas_call(
            mlp_kernel,
            out_shape=jax.ShapeDtypeStruct((rows, d), BF16),
            in_specs=[pl.BlockSpec(memory_space=pl.ANY)] * 4,
            out_specs=pl.BlockSpec(memory_space=pl.ANY),
            scratch_shapes=[
                pltpu.VMEM((2, R, d), BF16),
                pltpu.VMEM((2, d, 2 * TG), BF16),
                pltpu.VMEM((d // TD, ff, TD), BF16),
                pltpu.VMEM((R, ff), BF16),
                pltpu.VMEM((2, *chunk), F32),
                pltpu.VMEM((2, *chunk), BF16),
                pltpu.VMEM((4, *chunk), BF16),
                pltpu.VMEM((8, *chunk), BF16),
                pltpu.VMEM((8, *chunk), BF16),
                pltpu.VMEM((2, *chunk), BF16),
                dma((2,)), dma((2, 2)), dma((d // TD,)),
                dma((2,)), dma((4,)), dma((8,)), dma((8,)), dma((2,)), dma, dma((2,)),
                pltpu.SemaphoreType.REGULAR, pltpu.SemaphoreType.REGULAR,
            ],
            compiler_params=pltpu.CompilerParams(
                collective_id=0, has_side_effects=True, vmem_limit_bytes=67043328),
            cost_estimate=pl.CostEstimate(
                flops=6 * rows * d * ff, bytes_accessed=2 * (rows // R) * 2 * d * ff, transcendentals=rows * ff),
        )(x, w_gate, w_up, w_down)

    return jax.shard_map(
        step,
        mesh=mesh,
        in_specs=(P("dp", None), P(None, "tp"), P(None, "tp"), P("tp", None)),
        out_specs=P("dp", None),
        check_vma=False,
    )
```
